32 devices in a mesh: dp: 8 (over y, x, core), rep: 4 (over z).
Axes of the slice: x: 2, y: 2, z: 4, core: 2. Of those that a mesh axis runs over, the one named last changes fastest.
Arguments:
- student_in: bfloat16 [16384, 320], P(('dp', 'rep')), may hold values from -6 to 6
- target_in: bfloat16 [16384, 320], P(('dp', 'rep')), may hold values from -6 to 6
- timesteps: int32 [64], P(('dp', 'rep')), may hold values from 20 to 999
- student_win: float32 [1280, 320], P('dp'), may hold values from -0.3125 to 0.3125
- student_wout: float32 [640, 320], P('dp'), may hold values from -0.25 to 0.25
- student_wtime: float32 [640, 320], P('dp'), may hold values from -0.25 to 0.25
- student_gain: float32 [320], replicated, may hold values from 0.5 to 1.5
- student_bias: float32 [320], replicated, may hold values from -3 to 3
- target_win: float32 [1280, 320], P('dp'), may hold values from -0.3125 to 0.3125
- target_wout: float32 [640, 320], P('dp'), may hold values from -0.25 to 0.25
- target_wtime: float32 [640, 320], P('dp'), may hold values from -0.25 to 0.25
- target_gain: float32 [320], replicated, may hold values from 0.5 to 1.5
- target_bias: float32 [320], replicated, may hold values from -3 to 3
Outputs:
- grad_win: float32 [1280, 320], P('dp')
- grad_wout: float32 [640, 320], P('dp')
- grad_wtime: float32 [640, 320], P('dp')
- grad_gain: float32 [320], replicated
- grad_bias: float32 [320], replicated
- ema_win: float32 [1280, 320], P('dp')
- ema_wout: float32 [640, 320], P('dp')
- ema_wtime: float32 [640, 320], P('dp')
- ema_gain: float32 [320], replicated
- ema_bias: float32 [320], replicated
The draws below stay inside these ranges and needn't reach their ends.
Inputs may be any that keep to these rules, and one draw needn't show every extreme that they name: `timesteps`: student timestep of each sample; the target is evaluated at 20 steps earlier.
All inputs are finite; a program needn't handle non-finite values.
Results may differ from the reference program's by a relative error of at most 0.004.
The reference program's roundings to bfloat16 on the way (of `time_feat`, `normed_b`, `hidden`, `grad_yb` and `grad_mix`) count: a program that leaves them out, or rounds other values in their place, can miss the bound.
Values may be sent and summed in bfloat16 or wider, within the bound.
No kernel may reach another device: no remote copies, remote signals or barrier semaphores. Data moves between devices by JAX's collectives and lax.ppermute only.
A program may use at most 64 MiB of HBM per device.

```python
import math
import jax
import jax.numpy as jnp
from jax import lax

D = 320
FF = 640
TEMB = 640
SKIP = 20
TOK_DEV = 512
SAMPLES = 64
TOKENS = 16384
N_DP = 8


def set_ends(values, key, least, top_value):
    longest = values.shape.index(max(values.shape))
    spots = []
    for shift in (0, 1):
        where = [jax.random.randint(jax.random.fold_in(key, axis), (), 0, length) for axis, length in enumerate(values.shape)]
        where[longest] = (where[longest] + shift) % values.shape[longest]
        spots.append(tuple(where))
    return values.at[spots[0]].set(least).at[spots[1]].set(top_value)


def levels(stream_key, dims, split, least, largest):
    def one(axis_at, shards_of):
        steps = jax.random.uniform(jax.random.fold_in(jax.random.fold_in(stream_key, 6), axis_at), (shards_of,), jnp.float32, least / len(split), largest / len(split))
        return jnp.repeat(jnp.exp(steps), dims[axis_at] // shards_of).reshape((-1,) + (1,) * (len(dims) - axis_at - 1))

    level = one(*split[0])
    for cut in split[1:]:
        level = level * one(*cut)
    return level


def normal_values(own_key, extent, spread, most, shards=(), kind=jnp.bfloat16):
    values = spread * jax.random.normal(own_key, extent, jnp.float32)
    if shards:
        values = values * levels(own_key, extent, shards, -0.22, 0.18)
    return jnp.clip(values, -most, most).astype(kind)


def setup_inputs(seed: int = 0) -> dict:
    keys = jax.random.split(jax.random.key(seed), 14)
    return {
        "student_in": normal_values(keys[0], (TOKENS, D), 1.0, 6.0, ((0, 32),)),
        "target_in": normal_values(keys[1], (TOKENS, D), 1.0, 6.0, ((0, 32),)),
        "timesteps": set_ends(jax.random.randint(keys[2], (SAMPLES,), SKIP, 1000), jax.random.fold_in(keys[2], 1), SKIP, 999).astype(jnp.int32),
        "student_win": normal_values(keys[3], (2 * FF, D), D ** -0.5, 0.3125, ((0, 8),), jnp.float32),
        "student_wout": normal_values(keys[4], (FF, D), FF ** -0.5, 0.25, ((0, 8),), jnp.float32),
        "student_wtime": normal_values(keys[5], (TEMB, D), TEMB ** -0.5, 0.25, ((0, 8),), jnp.float32),
        "student_gain": jnp.clip(1.0 + 0.1 * jax.random.normal(keys[6], (D,), jnp.float32), 0.5, 1.5),
        "student_bias": normal_values(keys[7], (D,), 0.5, 3.0, (), jnp.float32),
        "target_win": normal_values(keys[8], (2 * FF, D), D ** -0.5, 0.3125, ((0, 8),), jnp.float32),
        "target_wout": normal_values(keys[9], (FF, D), FF ** -0.5, 0.25, ((0, 8),), jnp.float32),
        "target_wtime": normal_values(keys[10], (TEMB, D), TEMB ** -0.5, 0.25, ((0, 8),), jnp.float32),
        "target_gain": jnp.clip(1.0 + 0.1 * jax.random.normal(keys[11], (D,), jnp.float32), 0.5, 1.5),
        "target_bias": normal_values(keys[12], (D,), 0.5, 3.0, (), jnp.float32),
    }


ema_decay = 0.95
learn_rate = 0.05

def sinusoid(step_ids, width):
    half_width = width // 2
    frequency = jnp.exp(-math.log(10000.0) * jnp.arange(half_width, dtype=jnp.float32) / half_width)
    angles = step_ids.astype(jnp.float32)[:, None] * frequency[None, :]
    return jnp.concatenate([jnp.cos(angles), jnp.sin(angles)], axis=1)

def gelu_tanh(value):
    inner = 0.7978845608 * (value + 0.044715 * value * value * value)
    return 0.5 * value * (1.0 + jnp.tanh(inner))

def gelu_slope(value):
    tangent = jnp.tanh(0.7978845608 * (value + 0.044715 * value * value * value))
    return 0.5 * (1.0 + tangent) + 0.5 * value * (1.0 - tangent * tangent) * 0.7978845608 * (1.0 + 0.134145 * value * value)

def contract_last(left, right):
    return lax.dot_general(left, right, (((1,), (1,)), ((), ())), preferred_element_type=jnp.float32)

def contract_first(left, right):
    return lax.dot_general(left, right, (((0,), (0,)), ((), ())), preferred_element_type=jnp.float32)

def forward(tok_rows, step_ids, w_in, w_out, w_time, gain, bias):
    time_feat = jax.nn.silu(sinusoid(step_ids, w_time.shape[0])).astype(jnp.bfloat16)
    embedding = jnp.dot(time_feat, w_time, preferred_element_type=jnp.float32)
    samples = step_ids.shape[0]
    width = tok_rows.shape[1]
    summed = tok_rows.astype(jnp.float32).reshape(samples, -1, width) + embedding[:, None, :]
    summed = summed.reshape(-1, width)
    center = summed - lax.optimization_barrier(jnp.mean(summed, axis=1, keepdims=True))
    inv_std = lax.rsqrt(lax.optimization_barrier(jnp.mean(center * center, axis=1, keepdims=True)) + 1e-05)
    normed = center * inv_std
    normed_b = (normed * gain + bias).astype(jnp.bfloat16)
    mixed = contract_last(normed_b, w_in)
    hidden_count = w_out.shape[0]
    gate_part = mixed[:, :hidden_count]
    up_part = mixed[:, hidden_count:]
    gelu_gate = gelu_tanh(gate_part)
    hidden = (gelu_gate * up_part).astype(jnp.bfloat16)
    output = summed + jnp.dot(hidden, w_out, preferred_element_type=jnp.float32)
    return (output, (time_feat, normed, inv_std, normed_b, gate_part, up_part, gelu_gate, hidden))

def backward(grad_y, saved, w_in, w_out, gain):
    time_feat, normed, inv_std, normed_b, gate_part, up_part, gelu_gate, hidden = saved
    grad_yb = grad_y.astype(jnp.bfloat16)
    grad_h = contract_last(grad_yb, w_out)
    grad_mix = jnp.concatenate([grad_h * up_part * gelu_slope(gate_part), grad_h * gelu_gate], axis=1).astype(jnp.bfloat16)
    grad_z = jnp.dot(grad_mix, w_in, preferred_element_type=jnp.float32)
    grad_gain = lax.optimization_barrier(jnp.sum(grad_z * normed, axis=0))
    grad_bias = lax.optimization_barrier(jnp.sum(grad_z, axis=0))
    grad_n = grad_z * gain
    grad_s = grad_y + inv_std * (grad_n - lax.optimization_barrier(jnp.mean(grad_n, axis=1, keepdims=True)) - normed * lax.optimization_barrier(jnp.mean(grad_n * normed, axis=1, keepdims=True)))
    samples = time_feat.shape[0]
    grad_emb = lax.optimization_barrier(jnp.sum(grad_s.reshape(samples, -1, grad_s.shape[1]), axis=1))
    grad_time = lax.dot_general(time_feat.astype(jnp.float32), grad_emb, (((0,), (0,)), ((), ())), precision=lax.Precision.HIGHEST, preferred_element_type=jnp.float32)
    return (grad_yb, grad_mix, grad_gain, grad_bias, grad_time)

def reference(student_in, target_in, timesteps, student_win, student_wout, student_wtime, student_gain, student_bias, target_win, target_wout, target_wtime, target_gain, target_bias):
    s_in = student_win.astype(jnp.bfloat16)
    s_out = student_wout.astype(jnp.bfloat16)
    s_time = student_wtime.astype(jnp.bfloat16)
    t_in = target_win.astype(jnp.bfloat16)
    t_out = target_wout.astype(jnp.bfloat16)
    t_time = target_wtime.astype(jnp.bfloat16)
    width = student_in.shape[1]
    student_blocks = student_in.reshape(N_DP, -1, width)
    target_blocks = target_in.reshape(N_DP, -1, width)
    step_blocks = timesteps.reshape(N_DP, -1)

    def one_block(carry, block):
        s_rows, t_rows, step_ids = block
        student_out, saved = forward(s_rows, step_ids, s_in, s_out, s_time, student_gain, student_bias)
        target_out, unused = forward(t_rows, step_ids - SKIP, t_in, t_out, t_time, target_gain, target_bias)
        grad_y = (student_out - target_out) / TOK_DEV
        grad_yb, grad_mix, grad_gain, grad_bias, grad_time = backward(grad_y, saved, s_in, s_out, student_gain)
        grad_in = contract_first(grad_mix, saved[3])
        grad_out = contract_first(saved[7], grad_yb)
        totals = (carry[0] + grad_in, carry[1] + grad_out, carry[2] + grad_time, carry[3] + grad_gain, carry[4] + grad_bias)
        return (totals, None)
    start = (jnp.zeros(student_win.shape, jnp.float32), jnp.zeros(student_wout.shape, jnp.float32), jnp.zeros(student_wtime.shape, jnp.float32), jnp.zeros(student_gain.shape, jnp.float32), jnp.zeros(student_bias.shape, jnp.float32))
    totals, unused = lax.scan(one_block, start, (student_blocks, target_blocks, step_blocks))
    grad_win, grad_wout, grad_wtime, grad_gain, grad_bias = totals

    def average(target_p, student_p, grad_p):
        return ema_decay * target_p + (1.0 - ema_decay) * (student_p - learn_rate * grad_p)
    return (grad_win, grad_wout, grad_wtime, grad_gain, grad_bias, average(target_win, student_win, grad_win), average(target_wout, student_wout, grad_wout), average(target_wtime, student_wtime, grad_wtime), average(target_gain, student_gain, grad_gain), average(target_bias, student_bias, grad_bias))
```

```python
import math

import jax
import jax.numpy as jnp
from jax import lax
from jax.sharding import PartitionSpec as P

SKIP = 20


ema_decay = 0.95
learn_rate = 0.05


def gelu_tanh(value):
    inner = 0.7978845608 * (value + 0.044715 * value * value * value)
    return 0.5 * value * (1.0 + jnp.tanh(inner))


def gelu_slope(value):
    tangent = jnp.tanh(0.7978845608 * (value + 0.044715 * value * value * value))
    return 0.5 * (1.0 + tangent) + 0.5 * value * (1.0 - tangent * tangent) * 0.7978845608 * (
        1.0 + 0.134145 * value * value
    )


def contract_last(left, right):
    return lax.dot_general(
        left, right, (((1,), (1,)), ((), ())), preferred_element_type=jnp.float32
    )


def contract_first(left, right):
    return lax.dot_general(
        left, right, (((0,), (0,)), ((), ())), preferred_element_type=jnp.float32
    )


def tree_sum(parts):
    parts = list(parts)
    while len(parts) > 1:
        parts = [parts[i] + parts[i + 1] for i in range(0, len(parts) - 1, 2)] + parts[len(parts) - len(parts) % 2 :]
    return parts[0]


def exchange(x, axis, count, mask):
    return lax.ppermute(x, axis, [(i, i ^ mask) for i in range(count)])


def gather_rows(x, count, order):
    me = lax.axis_index("dp")
    done = []
    for bit in order:
        other = exchange(x, "dp", count, 1 << bit)
        mine_is_high = ((me >> bit) & 1) == 1
        low = jnp.where(mine_is_high, other, x)
        high = jnp.where(mine_is_high, x, other)
        x = jnp.stack([low, high], axis=sum(1 for b in done if b > bit))
        done.append(bit)
    return x


def gather_small(x, axis, count):
    return [x] + [exchange(x, axis, count, k) for k in range(1, count)]


def scatter_small(parts, count):
    kept = [parts[j] for j in range(0, count, 2)]
    sent = jnp.stack([parts[j + 1] for j in range(0, count, 2)])
    sent = exchange(sent, "dp", count, 1)
    kept = [kept[m] + sent[m] for m in range(count // 2)]
    return tree_sum([kept[0]] + [exchange(kept[m], "dp", count, 2 * m) for m in range(1, count // 2)])


def scatter_blocks(blocks, count):
    me = lax.axis_index("dp")
    core = me & 1
    pairs = blocks.reshape((count // 2, 2) + blocks.shape[1:])
    away = lax.dynamic_index_in_dim(pairs, 1 - core, axis=1, keepdims=False)
    keep = lax.dynamic_index_in_dim(pairs, core, axis=1, keepdims=False)
    chip = me >> 1
    keep = keep + exchange(away.astype(CORE_TYPE), "dp", count, 1).astype(jnp.float32)
    total = lax.dynamic_index_in_dim(keep, chip, axis=0, keepdims=False)
    for k in range(1, count // 2):
        part = lax.dynamic_index_in_dim(keep, chip ^ k, axis=0, keepdims=False).astype(jnp.bfloat16)
        total = total + exchange(part, "dp", count, 2 * k).astype(jnp.float32)
    return total


def sum_over_rep(x, count):
    me = lax.axis_index("rep")
    rows = x.shape[0] // count
    chunks = x.reshape((count, rows) + x.shape[1:])
    total = lax.dynamic_index_in_dim(chunks, me, axis=0, keepdims=False)
    for k in range(1, count):
        part = lax.dynamic_index_in_dim(chunks, me ^ k, axis=0, keepdims=False).astype(jnp.bfloat16)
        total = total + exchange(part, "rep", count, k).astype(jnp.float32)
    total = total.astype(jnp.bfloat16)
    got = gather_small(total, "rep", count)
    out = jnp.zeros((count, rows) + x.shape[1:], jnp.bfloat16)
    for k in range(count):
        out = lax.dynamic_update_index_in_dim(out, got[k], me ^ k, axis=0)
    return out.reshape(x.shape).astype(jnp.float32)


CORE_TYPE = jnp.bfloat16


def time_features(step_ids, rows, width):
    half_width = width // 2
    column = lax.axis_index("dp") * rows + jnp.arange(rows)
    is_cos = column < half_width
    index = jnp.where(is_cos, column, column - half_width).astype(jnp.float32)
    frequency = jnp.exp(-math.log(10000.0) * index / half_width)
    angles = step_ids.astype(jnp.float32)[:, None] * frequency[None, :]
    wave = jnp.where(is_cos[None, :], jnp.cos(angles), jnp.sin(angles))
    return jax.nn.silu(wave).astype(jnp.bfloat16)


def normalize(tok_rows, embedding, gain, bias):
    samples, width = embedding.shape
    summed = tok_rows.astype(jnp.float32).reshape(samples, -1, width) + embedding[:, None, :]
    summed = summed.reshape(-1, width)
    center = summed - jnp.mean(summed, axis=1, keepdims=True)
    inv_std = lax.rsqrt(jnp.mean(center * center, axis=1, keepdims=True) + 1e-05)
    normed = center * inv_std
    return summed, normed, inv_std, (normed * gain + bias).astype(jnp.bfloat16)


def make_per_device(n_dp, n_rep):
    paired = n_dp <= 8
    bits = n_dp.bit_length() - 1

    def gather_net(win, wout, order):
        rows = win.shape[0]
        width = win.shape[1]
        if not paired:
            return (
                lax.all_gather(win.astype(jnp.bfloat16), "dp", axis=0, tiled=True),
                lax.all_gather(wout.astype(jnp.bfloat16), "dp", axis=0, tiled=True),
            )
        both = jnp.concatenate([win.astype(jnp.bfloat16), wout.astype(jnp.bfloat16)])
        full = gather_rows(both, n_dp, order)
        full = full.reshape((n_dp,) + both.shape)
        return full[:, :rows].reshape(-1, width), full[:, rows:].reshape(-1, width)

    def per_device(
        student_in,
        target_in,
        timesteps,
        student_win,
        student_wout,
        student_wtime,
        student_gain,
        student_bias,
        target_win,
        target_wout,
        target_wtime,
        target_gain,
        target_bias,
    ):
        width = student_in.shape[1]
        samples = timesteps.shape[0]
        up = list(range(1, bits)) + [0]
        down = list(range(bits - 1, 0, -1)) + [0]
        if paired:
            ids = jnp.stack(gather_small(timesteps, "dp", n_dp)).reshape(-1)
        else:
            ids = lax.all_gather(timesteps, "dp", axis=0, tiled=True)
        s_in, s_out = gather_net(student_win, student_wout, up)
        t_in, t_out = gather_net(target_win, target_wout, down)
        t_rows = student_wtime.shape[0]
        s_feat = time_features(ids, t_rows, t_rows * n_dp)
        t_feat = time_features(ids - SKIP, t_rows, t_rows * n_dp)
        s_emb = jnp.dot(s_feat, student_wtime.astype(jnp.bfloat16), preferred_element_type=jnp.float32)
        t_emb = jnp.dot(t_feat, target_wtime.astype(jnp.bfloat16), preferred_element_type=jnp.float32)
        both = jnp.concatenate([s_emb.reshape(n_dp, samples, width), t_emb.reshape(n_dp, samples, width)], axis=1)
        if paired:
            both = scatter_small([both[j] for j in range(n_dp)], n_dp)
        else:
            both = lax.psum_scatter(both, "dp", scatter_dimension=0, tiled=True)[0]

        s_sum, normed, inv_std, normed_b = normalize(student_in, both[:samples], student_gain, student_bias)
        t_sum, _, _, t_normed_b = normalize(target_in, both[samples:], target_gain, target_bias)
        hidden_count = s_out.shape[0]
        mixed = contract_last(normed_b, s_in)
        gate_part = mixed[:, :hidden_count]
        up_part = mixed[:, hidden_count:]
        gelu_gate = gelu_tanh(gate_part)
        hidden = (gelu_gate * up_part).astype(jnp.bfloat16)
        student_out = s_sum + jnp.dot(hidden, s_out, preferred_element_type=jnp.float32)
        t_mixed = contract_last(t_normed_b, t_in)
        t_hidden = (gelu_tanh(t_mixed[:, :hidden_count]) * t_mixed[:, hidden_count:]).astype(jnp.bfloat16)
        target_out = t_sum + jnp.dot(t_hidden, t_out, preferred_element_type=jnp.float32)
        grad_y = (student_out - target_out) / student_in.shape[0]

        grad_yb = grad_y.astype(jnp.bfloat16)
        grad_wout = contract_first(hidden, grad_yb)
        grad_h = contract_last(grad_yb, s_out)
        grad_mix = jnp.concatenate(
            [grad_h * up_part * gelu_slope(gate_part), grad_h * gelu_gate], axis=1
        ).astype(jnp.bfloat16)
        grad_win = contract_first(grad_mix, normed_b)
        if paired:
            blocks = jnp.concatenate(
                [grad_win.reshape(n_dp, -1, width), grad_wout.reshape(n_dp, -1, width)], axis=1
            )
            shard = scatter_blocks(blocks, n_dp)
        else:
            shard = jnp.concatenate(
                [
                    lax.psum_scatter(grad_win, "dp", scatter_dimension=0, tiled=True),
                    lax.psum_scatter(grad_wout, "dp", scatter_dimension=0, tiled=True),
                ]
            )
        grad_z = jnp.dot(grad_mix, s_in, preferred_element_type=jnp.float32)
        grad_gain = jnp.sum(grad_z * normed, axis=0)
        grad_bias = jnp.sum(grad_z, axis=0)
        grad_n = grad_z * student_gain
        grad_s = grad_y + inv_std * (
            grad_n
            - jnp.mean(grad_n, axis=1, keepdims=True)
            - normed * jnp.mean(grad_n * normed, axis=1, keepdims=True)
        )
        grad_emb = jnp.sum(grad_s.reshape(samples, -1, width), axis=1)
        small = jnp.concatenate([grad_emb, grad_gain[None], grad_bias[None]])
        if paired:
            smalls = gather_small(small, "dp", n_dp)
        else:
            every = lax.all_gather(small, "dp")
            smalls = [every[j] for j in range(n_dp)]
        embs = jnp.stack([s[:samples] for s in smalls]).reshape(-1, width)
        grad_time = lax.dot_general(
            s_feat.astype(jnp.float32),
            embs,
            (((0,), (0,)), ((), ())),
            precision=lax.Precision.HIGHEST,
            preferred_element_type=jnp.float32,
        )
        affine = tree_sum([s[samples:] for s in smalls])
        affine = tree_sum(gather_small(affine, "rep", n_rep))
        total_gain, total_bias = affine[0], affine[1]
        joined = jnp.concatenate([shard, grad_time])
        if joined.shape[0] % (16 * n_rep) == 0 and paired:
            joined = sum_over_rep(joined, n_rep)
        else:
            joined = lax.psum(joined, "rep")
        in_rows = student_win.shape[0]
        out_rows = student_wout.shape[0]
        shard_in = joined[:in_rows]
        shard_out = joined[in_rows : in_rows + out_rows]
        shard_time = joined[in_rows + out_rows :]

        def average(target_p, student_p, grad_p):
            return ema_decay * target_p + (1.0 - ema_decay) * (student_p - learn_rate * grad_p)

        return (
            shard_in,
            shard_out,
            shard_time,
            total_gain,
            total_bias,
            average(target_win, student_win, shard_in),
            average(target_wout, student_wout, shard_out),
            average(target_wtime, student_wtime, shard_time),
            average(target_gain, student_gain, total_gain),
            average(target_bias, student_bias, total_bias),
        )

    return per_device


def solution(mesh):
    in_specs = (
        P(("dp", "rep"), None),
        P(("dp", "rep"), None),
        P(("dp", "rep")),
        P("dp", None),
        P("dp", None),
        P("dp", None),
        P(),
        P(),
        P("dp", None),
        P("dp", None),
        P("dp", None),
        P(),
        P(),
    )
    out_specs = (
        P("dp", None),
        P("dp", None),
        P("dp", None),
        P(),
        P(),
        P("dp", None),
        P("dp", None),
        P("dp", None),
        P(),
        P(),
    )
    return jax.shard_map(
        make_per_device(mesh.shape["dp"], mesh.shape["rep"]), mesh=mesh, in_specs=in_specs, out_specs=out_specs, check_vma=False
    )
```

```python
import math

import jax
import jax.numpy as jnp
from jax import lax
from jax.experimental import pallas as pl
from jax.experimental.pallas import tpu as pltpu
from jax.sharding import PartitionSpec as P

SKIP = 20


ema_decay = 0.95
learn_rate = 0.05


def sinusoid(step_ids, width):
    half_width = width // 2
    frequency = jnp.exp(-math.log(10000.0) * jnp.arange(half_width, dtype=jnp.float32) / half_width)
    angles = step_ids.astype(jnp.float32)[:, None] * frequency[None, :]
    return jnp.concatenate([jnp.cos(angles), jnp.sin(angles)], axis=1)


def gelu_tanh(value):
    inner = 0.7978845608 * (value + 0.044715 * value * value * value)
    return 0.5 * value * (1.0 + jnp.tanh(inner))


def gelu_slope(value):
    tangent = jnp.tanh(0.7978845608 * (value + 0.044715 * value * value * value))
    return 0.5 * (1.0 + tangent) + 0.5 * value * (1.0 - tangent * tangent) * 0.7978845608 * (
        1.0 + 0.134145 * value * value
    )


def contract_last(left, right):
    return lax.dot_general(
        left, right, (((1,), (1,)), ((), ())), preferred_element_type=jnp.float32
    )


def contract_first(left, right):
    return lax.dot_general(
        left, right, (((0,), (0,)), ((), ())), preferred_element_type=jnp.float32
    )


def forward(tok_rows, step_ids, w_in, w_out, w_time, gain, bias):
    time_feat = jax.nn.silu(sinusoid(step_ids, w_time.shape[0])).astype(jnp.bfloat16)
    embedding = jnp.dot(time_feat, w_time, preferred_element_type=jnp.float32)
    samples = step_ids.shape[0]
    width = tok_rows.shape[1]
    summed = tok_rows.astype(jnp.float32).reshape(samples, -1, width) + embedding[:, None, :]
    summed = summed.reshape(-1, width)
    center = summed - jnp.mean(summed, axis=1, keepdims=True)
    inv_std = lax.rsqrt(jnp.mean(center * center, axis=1, keepdims=True) + 1e-05)
    normed = center * inv_std
    normed_b = (normed * gain + bias).astype(jnp.bfloat16)
    mixed = contract_last(normed_b, w_in)
    hidden_count = w_out.shape[0]
    gate_part = mixed[:, :hidden_count]
    up_part = mixed[:, hidden_count:]
    gelu_gate = gelu_tanh(gate_part)
    hidden = (gelu_gate * up_part).astype(jnp.bfloat16)
    output = summed + jnp.dot(hidden, w_out, preferred_element_type=jnp.float32)
    return (output, (time_feat, normed, inv_std, normed_b, gate_part, up_part, gelu_gate, hidden))


def backward(grad_y, saved, w_in, w_out, gain):
    time_feat, normed, inv_std, normed_b, gate_part, up_part, gelu_gate, hidden = saved
    grad_yb = grad_y.astype(jnp.bfloat16)
    grad_h = contract_last(grad_yb, w_out)
    grad_mix = jnp.concatenate(
        [grad_h * up_part * gelu_slope(gate_part), grad_h * gelu_gate], axis=1
    ).astype(jnp.bfloat16)
    grad_z = jnp.dot(grad_mix, w_in, preferred_element_type=jnp.float32)
    grad_gain = jnp.sum(grad_z * normed, axis=0)
    grad_bias = jnp.sum(grad_z, axis=0)
    grad_n = grad_z * gain
    grad_s = grad_y + inv_std * (
        grad_n
        - jnp.mean(grad_n, axis=1, keepdims=True)
        - normed * jnp.mean(grad_n * normed, axis=1, keepdims=True)
    )
    samples = time_feat.shape[0]
    grad_emb = jnp.sum(grad_s.reshape(samples, -1, grad_s.shape[1]), axis=1)
    grad_time = lax.dot_general(
        time_feat.astype(jnp.float32),
        grad_emb,
        (((0,), (0,)), ((), ())),
        precision=lax.Precision.HIGHEST,
        preferred_element_type=jnp.float32,
    )
    return (grad_yb, grad_mix, grad_gain, grad_bias, grad_time)


def fetch(piece_in, piece_out, piece_time):
    return (
        lax.all_gather(piece_in, "dp", axis=0, tiled=True),
        lax.all_gather(piece_out, "dp", axis=0, tiled=True),
        lax.all_gather(piece_time, "dp", axis=0, tiled=True),
    )


def per_device(
    student_in,
    target_in,
    timesteps,
    student_win,
    student_wout,
    student_wtime,
    student_gain,
    student_bias,
    target_win,
    target_wout,
    target_wtime,
    target_gain,
    target_bias,
):
    s_in, s_out, s_time = fetch(
        student_win.astype(jnp.bfloat16),
        student_wout.astype(jnp.bfloat16),
        student_wtime.astype(jnp.bfloat16),
    )
    student_out, saved = forward(
        student_in, timesteps, s_in, s_out, s_time, student_gain, student_bias
    )
    t_in, t_out, t_time = fetch(
        target_win.astype(jnp.bfloat16),
        target_wout.astype(jnp.bfloat16),
        target_wtime.astype(jnp.bfloat16),
    )
    target_out, unused = forward(
        target_in, timesteps - SKIP, t_in, t_out, t_time, target_gain, target_bias
    )
    grad_y = (student_out - target_out) / student_in.shape[0]
    back_in, back_out = (
        lax.all_gather(student_win.astype(jnp.bfloat16), "dp", axis=0, tiled=True),
        lax.all_gather(student_wout.astype(jnp.bfloat16), "dp", axis=0, tiled=True),
    )
    grad_yb, grad_mix, grad_gain, grad_bias, grad_time = backward(
        grad_y, saved, back_in, back_out, student_gain
    )
    normed_b = saved[3]
    hidden = saved[7]
    part = grad_mix
    shard_in = lax.psum_scatter(
        contract_first(part, normed_b), "dp", scatter_dimension=0, tiled=True
    )
    part = hidden
    shard_out = lax.psum_scatter(
        contract_first(part, grad_yb), "dp", scatter_dimension=0, tiled=True
    )
    shard_time = lax.psum_scatter(grad_time, "dp", scatter_dimension=0, tiled=True)
    shard_in, shard_out, shard_time = lax.psum((shard_in, shard_out, shard_time), "rep")
    total_gain, total_bias = lax.psum((grad_gain, grad_bias), ("dp", "rep"))

    def average(target_p, student_p, grad_p):
        return ema_decay * target_p + (1.0 - ema_decay) * (student_p - learn_rate * grad_p)

    return (
        shard_in,
        shard_out,
        shard_time,
        total_gain,
        total_bias,
        average(target_win, student_win, shard_in),
        average(target_wout, student_wout, shard_out),
        average(target_wtime, student_wtime, shard_time),
        average(target_gain, student_gain, total_gain),
        average(target_bias, student_bias, total_bias),
    )


def exchange(x, axis, count, mask):
    return lax.ppermute(x, axis, [(i, i ^ mask) for i in range(count)])


def gather_doubling(x, count, order):
    masks = [0]
    for bit in order[:-1]:
        x = jnp.concatenate([x, exchange(x, "dp", count, 1 << bit)])
        masks = masks + [m ^ (1 << bit) for m in masks]
    return x, exchange(x, "dp", count, 1 << order[-1]), masks, 1 << order[-1]


def sum_over_rep(x, count):
    me = lax.axis_index("rep")
    rows = x.shape[0] // count
    chunk = lambda k: lax.dynamic_slice_in_dim(x, (me ^ k) * rows, rows, axis=0)
    total = chunk(0)
    for k in range(1, count):
        total = total + exchange(chunk(k).astype(jnp.bfloat16), "rep", count, k).astype(jnp.float32)
    total = total.astype(jnp.bfloat16)
    out = jnp.zeros(x.shape, jnp.float32)
    for k in range(count):
        got = exchange(total, "rep", count, k) if k else total
        out = lax.dynamic_update_slice_in_dim(out, got.astype(jnp.float32), (me ^ k) * rows, axis=0)
    return out


def step_kernel(sizes, s_masks, s_far, t_masks, t_far):
    count, in_rows, out_rows, time_rows, samples, tokens, width = sizes
    rows = in_rows + out_rows + time_rows
    hidden_count = out_rows * count

    def body(
        me_ref, s_tok, t_tok, s_feat, t_feat, s_feat_t, s_gain, s_bias, t_gain, t_bias,
        s_near_ref, s_far_ref, t_near_ref, t_far_ref,
        away_ref, keep_ref, affine_ref,
        sw_in, sw_out, sw_time, tw_in, tw_out, tw_time, g_in, g_out, g_time, s_emb, t_emb, emb_grad,
    ):
        me = me_ref[0]

        def place(ref, masks, flip, w_in, w_out, w_time):
            for p, mask in enumerate(masks):
                at = me ^ (mask ^ flip)
                base = p * rows
                w_in[pl.ds(pl.multiple_of(at * in_rows, 16), in_rows), :] = ref[base : base + in_rows, :]
                base = base + in_rows
                w_out[pl.ds(pl.multiple_of(at * out_rows, 16), out_rows), :] = ref[base : base + out_rows, :]
                base = base + out_rows
                w_time[pl.ds(pl.multiple_of(at * time_rows, 16), time_rows), :] = ref[base : base + time_rows, :]

        place(s_near_ref, s_masks, 0, sw_in, sw_out, sw_time)
        place(s_far_ref, s_masks, s_far, sw_in, sw_out, sw_time)
        place(t_near_ref, t_masks, 0, tw_in, tw_out, tw_time)
        place(t_far_ref, t_masks, t_far, tw_in, tw_out, tw_time)
        s_emb[...] = jnp.dot(s_feat[...], sw_time[...], preferred_element_type=jnp.float32)
        t_emb[...] = jnp.dot(t_feat[...], tw_time[...], preferred_element_type=jnp.float32)
        g_in[...] = jnp.zeros_like(g_in)
        g_out[...] = jnp.zeros_like(g_out)
        affine_ref[...] = jnp.zeros_like(affine_ref)

        def norm(tok, emb, gain, bias):
            summed = tok.astype(jnp.float32) + emb
            center = summed - jnp.mean(summed, axis=1, keepdims=True)
            inv_std = lax.rsqrt(jnp.mean(center * center, axis=1, keepdims=True) + 1e-05)
            normed = center * inv_std
            return summed, normed, inv_std, (normed * gain + bias).astype(jnp.bfloat16)

        for s in range(samples):
            at = slice(s * tokens, (s + 1) * tokens)
            t_sum, _, _, t_norm = norm(t_tok[at, :], t_emb[s : s + 1, :], t_gain[...], t_bias[...])
            t_mixed = contract_last(t_norm, tw_in[...])
            t_hidden = (gelu_tanh(t_mixed[:, :hidden_count]) * t_mixed[:, hidden_count:]).astype(jnp.bfloat16)
            t_res = t_sum + jnp.dot(t_hidden, tw_out[...], preferred_element_type=jnp.float32)
            s_sum, normed, inv_std, normed_b = norm(s_tok[at, :], s_emb[s : s + 1, :], s_gain[...], s_bias[...])
            mixed = contract_last(normed_b, sw_in[...])
            gate = mixed[:, :hidden_count]
            up = mixed[:, hidden_count:]
            tangent = jnp.tanh(0.7978845608 * (gate + 0.044715 * gate * gate * gate))
            gelu_gate = 0.5 * gate * (1.0 + tangent)
            slope = 0.5 * (1.0 + tangent) + 0.5 * gate * (1.0 - tangent * tangent) * 0.7978845608 * (
                1.0 + 0.134145 * gate * gate
            )
            hidden = (gelu_gate * up).astype(jnp.bfloat16)
            s_res = s_sum + jnp.dot(hidden, sw_out[...], preferred_element_type=jnp.float32)
            grad_y = (s_res - t_res) / (samples * tokens)
            grad_yb = grad_y.astype(jnp.bfloat16)
            g_out[...] += contract_first(hidden, grad_yb)
            grad_h = contract_last(grad_yb, sw_out[...])
            mix_gate = (grad_h * up * slope).astype(jnp.bfloat16)
            mix_up = (grad_h * gelu_gate).astype(jnp.bfloat16)
            g_in[:hidden_count, :] += contract_first(mix_gate, normed_b)
            g_in[hidden_count:, :] += contract_first(mix_up, normed_b)
            grad_z = jnp.dot(mix_gate, sw_in[:hidden_count, :], preferred_element_type=jnp.float32) + jnp.dot(
                mix_up, sw_in[hidden_count:, :], preferred_element_type=jnp.float32
            )
            affine_ref[0:1, :] += jnp.sum(grad_z * normed, axis=0, keepdims=True)
            affine_ref[1:2, :] += jnp.sum(grad_z, axis=0, keepdims=True)
            grad_n = grad_z * s_gain[...]
            grad_s = grad_y + inv_std * (
                grad_n
                - jnp.mean(grad_n, axis=1, keepdims=True)
                - normed * jnp.mean(grad_n * normed, axis=1, keepdims=True)
            )
            emb_grad[s : s + 1, :] = jnp.sum(grad_s, axis=0, keepdims=True)

        total = s_feat_t[:, 0:1] * emb_grad[0:1, :]
        for s in range(1, samples):
            total = total + s_feat_t[:, s : s + 1] * emb_grad[s : s + 1, :]
        g_time[...] = total

        for p in range(count // 2):
            for flip, out in ((0, keep_ref), (1, away_ref)):
                at = me ^ (2 * p + flip)
                base = p * rows
                for ref, size in ((g_in, in_rows), (g_out, out_rows), (g_time, time_rows)):
                    out[base : base + size, :] = ref[pl.ds(pl.multiple_of(at * size, 16), size), :].astype(out.dtype)
                    base = base + size

    vm = pl.BlockSpec(memory_space=pltpu.VMEM)
    f32, bf16 = jnp.float32, jnp.bfloat16
    half = count // 2 * rows
    return pl.pallas_call(
        body,
        in_specs=[pl.BlockSpec(memory_space=pltpu.SMEM)] + [vm] * 13,
        out_specs=[vm] * 3,
        out_shape=[
            jax.ShapeDtypeStruct((half, width), bf16),
            jax.ShapeDtypeStruct((half, width), f32),
            jax.ShapeDtypeStruct((8, width), f32),
        ],
        scratch_shapes=[
            pltpu.VMEM((in_rows * count, width), bf16),
            pltpu.VMEM((out_rows * count, width), bf16),
            pltpu.VMEM((time_rows * count, width), bf16),
            pltpu.VMEM((in_rows * count, width), bf16),
            pltpu.VMEM((out_rows * count, width), bf16),
            pltpu.VMEM((time_rows * count, width), bf16),
            pltpu.VMEM((in_rows * count, width), f32),
            pltpu.VMEM((out_rows * count, width), f32),
            pltpu.VMEM((time_rows * count, width), f32),
            pltpu.VMEM((16, width), f32),
            pltpu.VMEM((16, width), f32),
            pltpu.VMEM((8, width), f32),
        ],
        compiler_params=pltpu.CompilerParams(vmem_limit_bytes=48 * 1024 * 1024),
        name="distill_step",
    )


def make_paired(n_dp, n_rep):
    bits = n_dp.bit_length() - 1

    def paired(
        student_in,
        target_in,
        timesteps,
        student_win,
        student_wout,
        student_wtime,
        student_gain,
        student_bias,
        target_win,
        target_wout,
        target_wtime,
        target_gain,
        target_bias,
    ):
        width = student_in.shape[1]
        samples = timesteps.shape[0]
        in_rows, out_rows, time_rows = student_win.shape[0], student_wout.shape[0], student_wtime.shape[0]
        rows = in_rows + out_rows + time_rows
        up = list(range(1, bits)) + [0]
        down = list(range(bits - 1, 0, -1)) + [0]

        def net(win, wout, wtime, order):
            block = jnp.concatenate([win, wout, wtime]).astype(jnp.bfloat16)
            return gather_doubling(block, n_dp, order)

        s_near, s_far, s_masks, s_flip = net(student_win, student_wout, student_wtime, up)
        t_near, t_far, t_masks, t_flip = net(target_win, target_wout, target_wtime, down)

        def feats(ids):
            feat = jax.nn.silu(sinusoid(ids, time_rows * n_dp)).astype(jnp.bfloat16)
            return jnp.pad(feat, ((0, 16 - samples), (0, 0)))

        s_feat = feats(timesteps)
        t_feat = feats(timesteps - SKIP)
        kernel = step_kernel(
            (n_dp, in_rows, out_rows, time_rows, samples, student_in.shape[0] // samples, width),
            s_masks, s_flip, t_masks, t_flip,
        )
        away, keep, affine = kernel(
            lax.axis_index("dp").reshape(1),
            student_in, target_in, s_feat, t_feat, s_feat.astype(jnp.float32).T,
            student_gain[None], student_bias[None], target_gain[None], target_bias[None],
            s_near, s_far, t_near, t_far,
        )
        near = exchange(away, "dp", n_dp, 1)
        total = keep[:rows] + near[:rows].astype(jnp.float32)
        for k in range(1, n_dp // 2):
            at = slice(k * rows, (k + 1) * rows)
            part = (keep[at] + near[at].astype(jnp.float32)).astype(jnp.bfloat16)
            total = total + exchange(part, "dp", n_dp, 2 * k).astype(jnp.float32)
        affine = affine[:2]
        for bit in range(bits):
            affine = affine + exchange(affine, "dp", n_dp, 1 << bit)
        for bit in range(n_rep.bit_length() - 1):
            affine = affine + exchange(affine, "rep", n_rep, 1 << bit)
        total_gain, total_bias = affine[0], affine[1]
        total = sum_over_rep(total, n_rep)
        shard_in = total[:in_rows]
        shard_out = total[in_rows : in_rows + out_rows]
        shard_time = total[in_rows + out_rows :]

        def average(target_p, student_p, grad_p):
            return ema_decay * target_p + (1.0 - ema_decay) * (student_p - learn_rate * grad_p)

        return (
            shard_in,
            shard_out,
            shard_time,
            total_gain,
            total_bias,
            average(target_win, student_win, shard_in),
            average(target_wout, student_wout, shard_out),
            average(target_wtime, student_wtime, shard_time),
            average(target_gain, student_gain, total_gain),
            average(target_bias, student_bias, total_bias),
        )

    return paired


def solution(mesh):
    in_specs = (
        P(("dp", "rep"), None),
        P(("dp", "rep"), None),
        P(("dp", "rep")),
        P("dp", None),
        P("dp", None),
        P("dp", None),
        P(),
        P(),
        P("dp", None),
        P("dp", None),
        P("dp", None),
        P(),
        P(),
    )
    out_specs = (
        P("dp", None),
        P("dp", None),
        P("dp", None),
        P(),
        P(),
        P("dp", None),
        P("dp", None),
        P("dp", None),
        P(),
        P(),
    )
    n_dp, n_rep = mesh.shape["dp"], mesh.shape["rep"]
    body = make_paired(n_dp, n_rep) if n_dp <= 8 else per_device
    return jax.shard_map(
        body, mesh=mesh, in_specs=in_specs, out_specs=out_specs, check_vma=False
    )
```

```python
import math

import jax
import jax.numpy as jnp
from jax import lax
from jax.experimental import pallas as pl
from jax.experimental.layout import Layout, with_layout_constraint
from jax.experimental.pallas import tpu as pltpu
from jax.sharding import PartitionSpec as P

SKIP = 20


ema_decay = 0.95
learn_rate = 0.05


def sinusoid(step_ids, width):
    half_width = width // 2
    frequency = jnp.exp(-math.log(10000.0) * jnp.arange(half_width, dtype=jnp.float32) / half_width)
    angles = step_ids.astype(jnp.float32)[:, None] * frequency[None, :]
    return jnp.concatenate([jnp.cos(angles), jnp.sin(angles)], axis=1)


def gelu_tanh(value):
    inner = 0.7978845608 * (value + 0.044715 * value * value * value)
    return 0.5 * value * (1.0 + jnp.tanh(inner))


def gelu_slope(value):
    tangent = jnp.tanh(0.7978845608 * (value + 0.044715 * value * value * value))
    return 0.5 * (1.0 + tangent) + 0.5 * value * (1.0 - tangent * tangent) * 0.7978845608 * (
        1.0 + 0.134145 * value * value
    )


def contract_last(left, right):
    return lax.dot_general(
        left, right, (((1,), (1,)), ((), ())), preferred_element_type=jnp.float32
    )


def contract_first(left, right):
    return lax.dot_general(
        left, right, (((0,), (0,)), ((), ())), preferred_element_type=jnp.float32
    )


def forward(tok_rows, step_ids, w_in, w_out, w_time, gain, bias):
    time_feat = jax.nn.silu(sinusoid(step_ids, w_time.shape[0])).astype(jnp.bfloat16)
    embedding = jnp.dot(time_feat, w_time, preferred_element_type=jnp.float32)
    samples = step_ids.shape[0]
    width = tok_rows.shape[1]
    summed = tok_rows.astype(jnp.float32).reshape(samples, -1, width) + embedding[:, None, :]
    summed = summed.reshape(-1, width)
    center = summed - jnp.mean(summed, axis=1, keepdims=True)
    inv_std = lax.rsqrt(jnp.mean(center * center, axis=1, keepdims=True) + 1e-05)
    normed = center * inv_std
    normed_b = (normed * gain + bias).astype(jnp.bfloat16)
    mixed = contract_last(normed_b, w_in)
    hidden_count = w_out.shape[0]
    gate_part = mixed[:, :hidden_count]
    up_part = mixed[:, hidden_count:]
    gelu_gate = gelu_tanh(gate_part)
    hidden = (gelu_gate * up_part).astype(jnp.bfloat16)
    output = summed + jnp.dot(hidden, w_out, preferred_element_type=jnp.float32)
    return (output, (time_feat, normed, inv_std, normed_b, gate_part, up_part, gelu_gate, hidden))


def backward(grad_y, saved, w_in, w_out, gain):
    time_feat, normed, inv_std, normed_b, gate_part, up_part, gelu_gate, hidden = saved
    grad_yb = grad_y.astype(jnp.bfloat16)
    grad_h = contract_last(grad_yb, w_out)
    grad_mix = jnp.concatenate(
        [grad_h * up_part * gelu_slope(gate_part), grad_h * gelu_gate], axis=1
    ).astype(jnp.bfloat16)
    grad_z = jnp.dot(grad_mix, w_in, preferred_element_type=jnp.float32)
    grad_gain = jnp.sum(grad_z * normed, axis=0)
    grad_bias = jnp.sum(grad_z, axis=0)
    grad_n = grad_z * gain
    grad_s = grad_y + inv_std * (
        grad_n
        - jnp.mean(grad_n, axis=1, keepdims=True)
        - normed * jnp.mean(grad_n * normed, axis=1, keepdims=True)
    )
    samples = time_feat.shape[0]
    grad_emb = jnp.sum(grad_s.reshape(samples, -1, grad_s.shape[1]), axis=1)
    grad_time = lax.dot_general(
        time_feat.astype(jnp.float32),
        grad_emb,
        (((0,), (0,)), ((), ())),
        precision=lax.Precision.HIGHEST,
        preferred_element_type=jnp.float32,
    )
    return (grad_yb, grad_mix, grad_gain, grad_bias, grad_time)


def fetch(piece_in, piece_out, piece_time):
    return (
        lax.all_gather(piece_in, "dp", axis=0, tiled=True),
        lax.all_gather(piece_out, "dp", axis=0, tiled=True),
        lax.all_gather(piece_time, "dp", axis=0, tiled=True),
    )


def per_device(
    student_in,
    target_in,
    timesteps,
    student_win,
    student_wout,
    student_wtime,
    student_gain,
    student_bias,
    target_win,
    target_wout,
    target_wtime,
    target_gain,
    target_bias,
):
    s_in, s_out, s_time = fetch(
        student_win.astype(jnp.bfloat16),
        student_wout.astype(jnp.bfloat16),
        student_wtime.astype(jnp.bfloat16),
    )
    student_out, saved = forward(
        student_in, timesteps, s_in, s_out, s_time, student_gain, student_bias
    )
    t_in, t_out, t_time = fetch(
        target_win.astype(jnp.bfloat16),
        target_wout.astype(jnp.bfloat16),
        target_wtime.astype(jnp.bfloat16),
    )
    target_out, unused = forward(
        target_in, timesteps - SKIP, t_in, t_out, t_time, target_gain, target_bias
    )
    grad_y = (student_out - target_out) / student_in.shape[0]
    back_in, back_out = (
        lax.all_gather(student_win.astype(jnp.bfloat16), "dp", axis=0, tiled=True),
        lax.all_gather(student_wout.astype(jnp.bfloat16), "dp", axis=0, tiled=True),
    )
    grad_yb, grad_mix, grad_gain, grad_bias, grad_time = backward(
        grad_y, saved, back_in, back_out, student_gain
    )
    normed_b = saved[3]
    hidden = saved[7]
    part = grad_mix
    shard_in = lax.psum_scatter(
        contract_first(part, normed_b), "dp", scatter_dimension=0, tiled=True
    )
    part = hidden
    shard_out = lax.psum_scatter(
        contract_first(part, grad_yb), "dp", scatter_dimension=0, tiled=True
    )
    shard_time = lax.psum_scatter(grad_time, "dp", scatter_dimension=0, tiled=True)
    shard_in, shard_out, shard_time = lax.psum((shard_in, shard_out, shard_time), "rep")
    total_gain, total_bias = lax.psum((grad_gain, grad_bias), ("dp", "rep"))

    def average(target_p, student_p, grad_p):
        return ema_decay * target_p + (1.0 - ema_decay) * (student_p - learn_rate * grad_p)

    return (
        shard_in,
        shard_out,
        shard_time,
        total_gain,
        total_bias,
        average(target_win, student_win, shard_in),
        average(target_wout, student_wout, shard_out),
        average(target_wtime, student_wtime, shard_time),
        average(target_gain, student_gain, total_gain),
        average(target_bias, student_bias, total_bias),
    )


def row_major(x):
    return with_layout_constraint(x, Layout(major_to_minor=(0, 1)))


def exchange(x, axis, count, mask):
    return row_major(lax.ppermute(row_major(x), axis, [(i, i ^ mask) for i in range(count)]))


def gather_doubling(x, count, order):
    far = 1 << order[-1]
    pieces, masks, found = x, [0], []
    for bit in order[:-1]:
        got = exchange(pieces, "dp", count, 1 << bit)
        got_masks = [m ^ (1 << bit) for m in masks]
        if bit == order[-2]:
            found.append((pieces, masks))
            found.append((exchange(pieces, "dp", count, far), [m ^ far for m in masks]))
            found.append((got, got_masks))
            found.append((exchange(got, "dp", count, far), [m ^ far for m in got_masks]))
        else:
            pieces = jnp.concatenate([pieces, got])
            masks = masks + got_masks
    return [a for a, _ in found], [m for _, m in found]


def split_rows(x):
    high = x.astype(jnp.bfloat16)
    low = (x - high.astype(jnp.float32)).astype(jnp.bfloat16)
    return high, low, high.astype(jnp.float32) + low.astype(jnp.float32)


def put_affine(ref, base, high, low):
    pad = jnp.zeros((TAIL - 4, ref.shape[1]), jnp.float32)
    rows = jnp.concatenate([high.astype(jnp.float32), low.astype(jnp.float32), pad], axis=0)
    ref[base : base + TAIL, :] = rows.astype(jnp.bfloat16)


def get_affine(ref, base):
    rows = ref[base : base + TAIL, :].astype(jnp.float32)
    return rows[0:2, :] + rows[2:4, :]


def tree_sum(parts):
    while len(parts) > 1:
        parts = [parts[i] + parts[i + 1] for i in range(0, len(parts), 2)]
    return parts[0]


TAIL = 16
SMALL = pltpu.CompilerParams(vmem_limit_bytes=8 * 1024 * 1024)
VM = pl.BlockSpec(memory_space=pltpu.VMEM)
SM = pl.BlockSpec(memory_space=pltpu.SMEM)


def call(body, name, outs, inputs, scalars=0):
    return pl.pallas_call(
        body,
        in_specs=[SM] * scalars + [VM] * (len(inputs) - scalars),
        out_specs=[VM] * len(outs),
        out_shape=[jax.ShapeDtypeStruct(shape, dtype) for shape, dtype in outs],
        compiler_params=SMALL,
        name=name,
    )(*inputs)


def chip_sums(keep, near, near_two, affine, rows, parts):
    width = keep.shape[1]

    split = parts // 2

    def body(keep_ref, near_ref, two_ref, affine_ref, own_ref, held_ref, *sent):
        own_ref[...] = keep_ref[:rows, :] + near_ref[:rows, :].astype(jnp.float32)
        high, low, value = split_rows(affine_ref[0:2, :] + get_affine(near_ref, split * rows))
        held_ref[...] = jnp.zeros_like(held_ref)
        held_ref[0:2, :] = value
        for k in range(1, parts):
            at = slice(k * rows, (k + 1) * rows)
            ref = near_ref if k < split else two_ref
            base = (k if k < split else k - split) * rows
            sent[k - 1][:rows, :] = (keep_ref[at, :] + ref[base : base + rows, :].astype(jnp.float32)).astype(jnp.bfloat16)
            put_affine(sent[k - 1], rows, high, low)

    outs = [((rows, width), jnp.float32), ((8, width), jnp.float32)]
    outs += [((rows + TAIL, width), jnp.bfloat16)] * (parts - 1)
    return call(body, "chip_sums", outs, [keep, near, near_two, affine])


def plane_sums(me, own, held, got, parts):
    rows, width = own.shape
    size = rows // parts
    n_got = len(got)

    def body(me_ref, own_ref, held_ref, *refs):
        got_refs, (mine_ref, next_ref), sent, (scratch,) = (
            refs[:n_got], refs[n_got : n_got + 2], refs[n_got + 2 : -1], refs[-1:]
        )
        total = own_ref[...]
        for ref in got_refs:
            total = total + ref[:rows, :].astype(jnp.float32)
        scratch[...] = total
        summed = tree_sum([held_ref[0:2, :]] + [get_affine(ref, rows) for ref in got_refs])
        high, low, value = split_rows(summed)
        next_ref[...] = jnp.zeros_like(next_ref)
        next_ref[0:2, :] = value
        mine_ref[...] = scratch[pl.ds(pl.multiple_of(me_ref[0] * size, 8), size), :]
        for k in range(1, parts):
            at = pl.multiple_of((me_ref[0] ^ k) * size, 8)
            sent[k - 1][:size, :] = scratch[pl.ds(at, size), :].astype(jnp.bfloat16)
            put_affine(sent[k - 1], size, high, low)

    outs = [((size, width), jnp.float32), ((8, width), jnp.float32)]
    outs += [((size + TAIL, width), jnp.bfloat16)] * (parts - 1)
    return pl.pallas_call(
        body,
        in_specs=[SM] + [VM] * (2 + n_got),
        out_specs=[VM] * len(outs),
        out_shape=[jax.ShapeDtypeStruct(shape, dtype) for shape, dtype in outs],
        scratch_shapes=[pltpu.VMEM((rows, width), jnp.float32)],
        compiler_params=SMALL,
        name="plane_sums",
    )(me, own, held, *got)


def line_sums(mine, held, got):
    size, width = mine.shape

    def body(mine_ref, held_ref, *refs):
        got_refs, (total_ref, affine_ref) = refs[:-2], refs[-2:]
        total = mine_ref[...]
        for ref in got_refs:
            total = total + ref[:size, :].astype(jnp.float32)
        total_ref[...] = total.astype(jnp.bfloat16)
        affine_ref[...] = jnp.zeros_like(affine_ref)
        affine_ref[0:2, :] = tree_sum([held_ref[0:2, :]] + [get_affine(ref, size) for ref in got_refs])

    outs = [((size, width), jnp.bfloat16), ((8, width), jnp.float32)]
    return call(body, "line_sums", outs, [mine, held] + list(got))


def finish(me, pieces, students, targets):
    size, width = pieces[0].shape
    n_pieces = len(pieces)
    n_nets = len(students)

    def body(me_ref, *refs):
        piece_refs = refs[:n_pieces]
        s_refs = refs[n_pieces : n_pieces + n_nets]
        t_refs = refs[n_pieces + n_nets : n_pieces + 2 * n_nets]
        grads = refs[n_pieces + 2 * n_nets : n_pieces + 3 * n_nets]
        news = refs[n_pieces + 3 * n_nets : n_pieces + 4 * n_nets]
        scratch = refs[-1]
        for k, ref in enumerate(piece_refs):
            scratch[pl.ds(pl.multiple_of((me_ref[0] ^ k) * size, 8), size), :] = ref[...].astype(jnp.float32)
        base = 0
        for s_ref, t_ref, g_ref, n_ref in zip(s_refs, t_refs, grads, news):
            grad = scratch[base : base + s_ref.shape[0], :]
            base = base + s_ref.shape[0]
            g_ref[...] = grad
            n_ref[...] = ema_decay * t_ref[...] + (1.0 - ema_decay) * (s_ref[...] - learn_rate * grad)

    outs = [jax.ShapeDtypeStruct(s.shape, jnp.float32) for s in students] * 2
    return pl.pallas_call(
        body,
        in_specs=[SM] + [VM] * (n_pieces + 2 * n_nets),
        out_specs=[VM] * len(outs),
        out_shape=outs,
        scratch_shapes=[pltpu.VMEM((size * n_pieces, width), jnp.float32)],
        compiler_params=SMALL,
        name="finish",
    )(me, *pieces, *students, *targets)


def step_kernel(sizes, s_masks, t_masks):
    count, in_rows, out_rows, time_rows, samples, tokens, width = sizes
    rows = in_rows + out_rows + time_rows
    hidden_count = out_rows * count
    n_pieces = len(s_masks) + len(t_masks)
    split = count // 4

    def body(
        me_ref, s_tok, t_tok, s_feat, t_feat, s_gain, s_bias, t_gain, t_bias, *rest
    ):
        s_refs, t_refs, rest = rest[: len(s_masks)], rest[len(s_masks) : n_pieces], rest[n_pieces:]
        (
            away_ref, away_two_ref, keep_ref, affine_ref, sw_in, sw_out, sw_time, tw_in, tw_out, tw_time, g_in, g_out, g_time, s_emb, t_emb, emb_grad, affine,
        ) = rest
        me = me_ref[0]

        def place(ref, masks, w_in, w_out, w_time):
            for p, mask in enumerate(masks):
                at = me ^ mask
                base = p * rows
                w_in[pl.ds(pl.multiple_of(at * in_rows, 16), in_rows), :] = ref[base : base + in_rows, :]
                base = base + in_rows
                w_out[pl.ds(pl.multiple_of(at * out_rows, 16), out_rows), :] = ref[base : base + out_rows, :]
                base = base + out_rows
                w_time[pl.ds(pl.multiple_of(at * time_rows, 16), time_rows), :] = ref[base : base + time_rows, :]

        for ref, masks in zip(s_refs, s_masks):
            place(ref, masks, sw_in, sw_out, sw_time)
        for ref, masks in zip(t_refs, t_masks):
            place(ref, masks, tw_in, tw_out, tw_time)
        s_emb[...] = jnp.dot(s_feat[...], sw_time[...], preferred_element_type=jnp.float32)
        t_emb[...] = jnp.dot(t_feat[...], tw_time[...], preferred_element_type=jnp.float32)
        g_in[...] = jnp.zeros_like(g_in)
        g_out[...] = jnp.zeros_like(g_out)
        affine[...] = jnp.zeros_like(affine)
        emb_grad[...] = jnp.zeros_like(emb_grad)

        def norm(tok, emb, gain, bias):
            summed = tok.astype(jnp.float32) + emb
            center = summed - jnp.mean(summed, axis=1, keepdims=True)
            inv_std = lax.rsqrt(jnp.mean(center * center, axis=1, keepdims=True) + 1e-05)
            normed = center * inv_std
            return summed, normed, inv_std, (normed * gain + bias).astype(jnp.bfloat16)

        for s in range(samples):
            at = slice(s * tokens, (s + 1) * tokens)
            t_sum, _, _, t_norm = norm(t_tok[:, at].T, t_emb[s : s + 1, :], t_gain[...], t_bias[...])
            t_mixed = contract_last(t_norm, tw_in[...])
            t_hidden = (gelu_tanh(t_mixed[:, :hidden_count]) * t_mixed[:, hidden_count:]).astype(jnp.bfloat16)
            t_res = t_sum + jnp.dot(t_hidden, tw_out[...], preferred_element_type=jnp.float32)
            s_sum, normed, inv_std, normed_b = norm(s_tok[:, at].T, s_emb[s : s + 1, :], s_gain[...], s_bias[...])
            mixed = contract_last(normed_b, sw_in[...])
            gate = mixed[:, :hidden_count]
            up = mixed[:, hidden_count:]
            tangent = jnp.tanh(0.7978845608 * (gate + 0.044715 * gate * gate * gate))
            gelu_gate = 0.5 * gate * (1.0 + tangent)
            slope = 0.5 * (1.0 + tangent) + 0.5 * gate * (1.0 - tangent * tangent) * 0.7978845608 * (
                1.0 + 0.134145 * gate * gate
            )
            hidden = (gelu_gate * up).astype(jnp.bfloat16)
            s_res = s_sum + jnp.dot(hidden, sw_out[...], preferred_element_type=jnp.float32)
            grad_y = (s_res - t_res) / (samples * tokens)
            grad_yb = grad_y.astype(jnp.bfloat16)
            g_out[...] += contract_first(hidden, grad_yb)
            grad_h = contract_last(grad_yb, sw_out[...])
            mix_gate = (grad_h * up * slope).astype(jnp.bfloat16)
            mix_up = (grad_h * gelu_gate).astype(jnp.bfloat16)
            g_in[:hidden_count, :] += contract_first(mix_gate, normed_b)
            g_in[hidden_count:, :] += contract_first(mix_up, normed_b)
            grad_z = jnp.dot(mix_gate, sw_in[:hidden_count, :], preferred_element_type=jnp.float32) + jnp.dot(
                mix_up, sw_in[hidden_count:, :], preferred_element_type=jnp.float32
            )
            affine[0:1, :] += jnp.sum(grad_z * normed, axis=0, keepdims=True)
            affine[1:2, :] += jnp.sum(grad_z, axis=0, keepdims=True)
            grad_n = grad_z * s_gain[...]
            grad_s = grad_y + inv_std * (
                grad_n
                - jnp.mean(grad_n, axis=1, keepdims=True)
                - normed * jnp.mean(grad_n * normed, axis=1, keepdims=True)
            )
            emb_grad[s : s + 1, :] = jnp.sum(grad_s, axis=0, keepdims=True)

        rest_of = emb_grad[...]
        total = jnp.zeros(g_time.shape, jnp.float32)
        for _ in range(3):
            piece = rest_of.astype(jnp.bfloat16)
            rest_of = rest_of - piece.astype(jnp.float32)
            total = total + contract_first(s_feat[...], piece)
        g_time[...] = total
        high, low, value = split_rows(affine[0:2, :])
        affine_ref[...] = jnp.zeros_like(affine_ref)
        affine_ref[0:2, :] = value
        put_affine(away_ref, split * rows, high, low)

        for p in range(count // 2):
            for flip, out in ((0, keep_ref), (1, away_ref)):
                at = me ^ (2 * p + flip)
                base = p * rows
                if flip and p >= split:
                    out, base = away_two_ref, (p - split) * rows
                for ref, size in ((g_in, in_rows), (g_out, out_rows), (g_time, time_rows)):
                    out[base : base + size, :] = ref[pl.ds(pl.multiple_of(at * size, 16), size), :].astype(out.dtype)
                    base = base + size

    vm = pl.BlockSpec(memory_space=pltpu.VMEM)
    f32, bf16 = jnp.float32, jnp.bfloat16
    half = count // 2 * rows
    return pl.pallas_call(
        body,
        in_specs=[pl.BlockSpec(memory_space=pltpu.SMEM)] + [vm] * (8 + n_pieces),
        out_specs=[vm] * 4,
        out_shape=[
            jax.ShapeDtypeStruct((split * rows + TAIL, width), bf16),
            jax.ShapeDtypeStruct((half - split * rows, width), bf16),
            jax.ShapeDtypeStruct((half, width), f32),
            jax.ShapeDtypeStruct((8, width), f32),
        ],
        scratch_shapes=[
            pltpu.VMEM((in_rows * count, width), bf16),
            pltpu.VMEM((out_rows * count, width), bf16),
            pltpu.VMEM((time_rows * count, width), bf16),
            pltpu.VMEM((in_rows * count, width), bf16),
            pltpu.VMEM((out_rows * count, width), bf16),
            pltpu.VMEM((time_rows * count, width), bf16),
            pltpu.VMEM((in_rows * count, width), f32),
            pltpu.VMEM((out_rows * count, width), f32),
            pltpu.VMEM((time_rows * count, width), f32),
            pltpu.VMEM((16, width), f32),
            pltpu.VMEM((16, width), f32),
            pltpu.VMEM((16, width), f32),
            pltpu.VMEM((8, width), f32),
        ],
        compiler_params=pltpu.CompilerParams(vmem_limit_bytes=28 * 1024 * 1024),
        name="distill_step",
    )


def make_paired(n_dp, n_rep):
    bits = n_dp.bit_length() - 1

    def paired(
        student_in,
        target_in,
        timesteps,
        student_win,
        student_wout,
        student_wtime,
        student_gain,
        student_bias,
        target_win,
        target_wout,
        target_wtime,
        target_gain,
        target_bias,
    ):
        width = student_in.shape[1]
        samples = timesteps.shape[0]
        in_rows, out_rows, time_rows = student_win.shape[0], student_wout.shape[0], student_wtime.shape[0]
        rows = in_rows + out_rows + time_rows
        up = list(range(1, bits)) + [0]
        down = list(range(bits - 1, 0, -1)) + [0]

        def net(win, wout, wtime, order):
            block = jnp.concatenate([win, wout, wtime]).astype(jnp.bfloat16)
            return gather_doubling(block, n_dp, order)

        s_pieces, s_masks = net(student_win, student_wout, student_wtime, up)
        t_pieces, t_masks = net(target_win, target_wout, target_wtime, down)

        def feats(ids):
            feat = jax.nn.silu(sinusoid(ids, time_rows * n_dp)).astype(jnp.bfloat16)
            return jnp.pad(feat, ((0, 16 - samples), (0, 0)))

        s_feat = feats(timesteps)
        t_feat = feats(timesteps - SKIP)
        kernel = step_kernel(
            (n_dp, in_rows, out_rows, time_rows, samples, student_in.shape[0] // samples, width),
            s_masks, t_masks,
        )
        away, away_two, keep, affine = kernel(
            lax.axis_index("dp").reshape(1),
            student_in.T, target_in.T, s_feat, t_feat,
            student_gain[None], student_bias[None], target_gain[None], target_bias[None],
            *s_pieces, *t_pieces,
        )
        near = exchange(away, "dp", n_dp, 1)
        near_two = exchange(away_two, "dp", n_dp, 1)
        own, held, *sent = chip_sums(keep, near, near_two, affine, rows, n_dp // 2)
        got = [exchange(part, "dp", n_dp, 2 * k) for k, part in enumerate(sent, 1)]
        rep_me = lax.axis_index("rep").reshape(1)
        mine, held, *sent = plane_sums(rep_me, own, held, got, n_rep)
        got = [exchange(part, "rep", n_rep, k) for k, part in enumerate(sent, 1)]
        total, held = line_sums(mine, held, got)
        pieces = [total] + [exchange(total, "rep", n_rep, k) for k in range(1, n_rep)]
        total_gain, total_bias = held[0], held[1]
        shard_in, shard_out, shard_time, new_in, new_out, new_time = finish(
            rep_me, pieces, [student_win, student_wout, student_wtime], [target_win, target_wout, target_wtime]
        )

        def average(target_p, student_p, grad_p):
            return ema_decay * target_p + (1.0 - ema_decay) * (student_p - learn_rate * grad_p)

        return (
            shard_in,
            shard_out,
            shard_time,
            total_gain,
            total_bias,
            new_in,
            new_out,
            new_time,
            average(target_gain, student_gain, total_gain),
            average(target_bias, student_bias, total_bias),
        )

    return paired


def solution(mesh):
    in_specs = (
        P(("dp", "rep"), None),
        P(("dp", "rep"), None),
        P(("dp", "rep")),
        P("dp", None),
        P("dp", None),
        P("dp", None),
        P(),
        P(),
        P("dp", None),
        P("dp", None),
        P("dp", None),
        P(),
        P(),
    )
    out_specs = (
        P("dp", None),
        P("dp", None),
        P("dp", None),
        P(),
        P(),
        P("dp", None),
        P("dp", None),
        P("dp", None),
        P(),
        P(),
    )
    n_dp, n_rep = mesh.shape["dp"], mesh.shape["rep"]
    body = make_paired(n_dp, n_rep) if n_dp <= 8 else per_device
    return jax.shard_map(
        body, mesh=mesh, in_specs=in_specs, out_specs=out_specs, check_vma=False
    )
```
